256 devices in a mesh: reps: 4 (over x, y), grow: 64 (over z, core).
Axes of the slice: x: 2, y: 2, z: 32, core: 2. Of those that a mesh axis runs over, the one named last changes fastest.
The devices are a block of a 4x8x32 slice.
Arguments:
- hamiltonian: float32 [1536, 3, 256, 256], P(('reps', 'grow')), parts along dimension 0, may hold values from -3 to 3, as said below
- pattern: int32 [384, 3], replicated, may hold values from 0 to 1, as said below
- potential: float32 [4], P('reps'), parts along dimension 0, may hold values from -0.2 to 0.2
Outputs:
- sign_matrix: float32 [1536, 3, 256, 256], P(('reps', 'grow')), parts along dimension 0
- occupation: float32 [4], P('reps'), parts along dimension 0
The draws below stay inside these ranges and needn't reach their ends.
There are 4 independent parts, one for each index of `reps`. The reference program is written for one: setup_inputs(seed, part) draws one part's arguments, and reference() takes and returns one part's arrays. A program takes and returns all parts, laid end to end along the dimension named above; an argument that names none is the same for every part. Nothing has to cross between parts.
Inputs may be any that keep to these rules, and one draw needn't show every extreme that they name: `hamiltonian`: the matrix is symmetric: slot 2 of block row i is the transpose of slot 0 of block row i + 1, slot 1 is symmetric, slot 0 of row 0 and slot 2 of row 383 are zero. pattern[i, 1] = 1; pattern[i, 2] = pattern[i + 1, 0]; pattern[0, 0] = pattern[383, 2] = 0.
All inputs are finite; a program needn't handle non-finite values.
Results may differ from the reference program's by a relative error of at most 0.0001.
Values sent between devices are 32-bit elements; how exact they have to be, the bound alone decides.
A program may use at most 64 MiB of HBM per device.

```python
import math
import jax
import jax.numpy as jnp
from jax import lax

BS = 256
ROWS_DEV = 6
ITERS = 2
NBLK = 384


def draw_hamiltonian(key, part):
    key_diag, key_rough, key_upper = jax.random.split(key, 3)
    spread = 0.25 / math.sqrt(3.0 * BS)
    levels = jnp.arange(NBLK, dtype=jnp.float32)
    centre = 0.5 - levels / max(NBLK - 1, 1)
    inner_raw = jax.random.normal(key_diag, (NBLK, BS, BS), jnp.float32) * spread
    upper_raw = jax.random.normal(key_upper, (NBLK, BS, BS), jnp.float32) * spread
    roughness = jax.random.uniform(key_rough, (NBLK, BS), jnp.float32, -0.3, 0.3)
    unit_block = jnp.eye(BS, dtype=jnp.float32)
    diagonal = (inner_raw + jnp.swapaxes(inner_raw, 1, 2)) * 0.7071 + (centre[:, None] + roughness)[:, :, None] * unit_block[None]
    zero_block = jnp.zeros((1, BS, BS), jnp.float32)
    below_block = jnp.concatenate([zero_block, jnp.swapaxes(upper_raw[:-1], 1, 2)], axis=0)
    above_block = jnp.concatenate([upper_raw[:-1], zero_block], axis=0)
    return jnp.stack([below_block, diagonal, above_block], axis=1)


def draw_pattern(key, part):
    choose = jax.random.randint(key, (NBLK - 1,), 0, 5)
    lower_row = jnp.arange(1, NBLK, dtype=jnp.int32)
    boundary = (lower_row % ROWS_DEV == 0).astype(jnp.int32)
    edge_kept = jnp.maximum((choose < 3).astype(jnp.int32), boundary)
    nothing = jnp.zeros((1,), jnp.int32)
    return jnp.stack([jnp.concatenate([nothing, edge_kept]), jnp.ones((NBLK,), jnp.int32), jnp.concatenate([edge_kept, nothing])], axis=1)


def setup_inputs(seed: int = 0, part: int = 0) -> dict:
    seeds = jax.random.split(jax.random.key(seed), 4)
    part_splits = jax.random.split(jax.random.fold_in(seeds[3], part), 4)
    hamiltonian = draw_hamiltonian(jax.random.fold_in(jax.random.fold_in(seeds[3], part), 71), part)
    pattern = draw_pattern(jax.random.fold_in(seeds[3], 71), part)
    potential = jnp.clip(jax.random.uniform(part_splits[2], (1,), jnp.float32, -0.2, 0.2), -0.2, 0.2)
    return dict(hamiltonian=hamiltonian, pattern=pattern, potential=potential)


def banded(operand, extended, keep_mask):
    row_count = operand.shape[0]
    columns = []
    for column in range(3):
        summed = jnp.zeros_like(operand[:, 0])
        for source in range(3):
            partner = column - source + 1
            if 0 <= partner < 3:
                summed = summed + jnp.einsum("rij,rjk->rik", operand[:, source], extended[source:source + row_count, partner], precision=lax.Precision.HIGHEST)
        columns.append(summed)
    return jnp.stack(columns, axis=1) * keep_mask[:, :, None, None]


def padded_rows(field):
    return jnp.pad(field, ((1, 1), (0, 0), (0, 0), (0, 0)))


def reference(hamiltonian, pattern, potential):
    keep_mask = pattern.astype(jnp.float32)
    unit_block = jnp.eye(BS, dtype=jnp.float32)
    slot_weight = (jnp.arange(3) == 1).astype(jnp.float32)
    identity_band = slot_weight[None, :, None, None] * unit_block[None, None]
    current = (potential[0] * identity_band - hamiltonian) * keep_mask[:, :, None, None]
    for iteration in range(ITERS):
        square = banded(current, padded_rows(current), keep_mask)
        shifted = (3.0 * identity_band - square) * keep_mask[:, :, None, None]
        current = 0.5 * banded(current, padded_rows(shifted), keep_mask)
    total_trace = jnp.sum(jnp.trace(current[:, 1], axis1=1, axis2=2))
    matrix_order = float(NBLK * BS)
    occupation = ((matrix_order + total_trace) / (2.0 * matrix_order)).reshape(1)
    return current, occupation
```

```python
import functools

import jax
import jax.numpy as jnp
from jax import lax
from jax.experimental import pallas as pl
from jax.experimental.pallas import tpu as pltpu
from jax.sharding import PartitionSpec as P

MESH = pl.DeviceIdType.MESH
F32 = jnp.float32
BF16 = jnp.bfloat16
STRIP = 32


def kernel(
    n_grow,
    pattern,
    potential,
    h_hbm,
    out,
    occupation,
    h,
    c_hi,
    c_lo,
    s_hi,
    s_lo,
    d_hi,
    d_lo,
    t_hi,
    t_lo,
    halo,
    edge,
    part,
    mate,
    slots,
    load_sem,
    send_sem,
    recv_sem,
    trace_send,
    trace_recv,
    known_sem,
):
    rows, edge_size = h.shape[0], h.shape[2]
    n_chips = n_grow // 2
    last = rows - 1
    me = lax.axis_index("grow")
    chip = me // 2
    mate_id = me + 1 - 2 * lax.rem(me, 2)

    def at(distance):
        return {"grow": lax.rem(me + distance + n_grow, n_grow)}

    loads = {}
    for i in (0, last, 1, last - 1, 2, 3):
        loads[i] = pltpu.make_async_copy(h_hbm.at[i], h.at[i], load_sem.at[i])
        loads[i].start()
    barrier = pltpu.get_barrier_semaphore()
    near = (1, -1, 2, -2, 4, -4)
    for distance in near:
        pl.semaphore_signal(barrier, inc=1, device_id=at(distance), device_id_type=MESH)
    pl.semaphore_wait(barrier, len(near))
    reaches = []
    reach = 2
    while reach < n_chips // 2:
        reaches.append(reach)
        reach *= 2

    def tell(step):
        if step >= len(reaches):
            return
        for distance in (2 * reaches[step], -2 * reaches[step]):
            pl.semaphore_signal(
                known_sem.at[step], inc=1, device_id=at(distance), device_id_type=MESH
            )

    def hear(step):
        if step >= len(reaches):
            return
        pl.semaphore_wait(known_sem.at[step], 2)

    tell(0)

    def exchange(k, first, second):
        copies = []
        for side, source, distance in ((1, first, -1), (0, second, 1)):
            copies.append(
                pltpu.make_async_remote_copy(
                    src_ref=source,
                    dst_ref=halo.at[k, side],
                    send_sem=send_sem.at[k, side],
                    recv_sem=recv_sem.at[k, side],
                    device_id=at(distance),
                    device_id_type=MESH,
                )
            )
        for copy in copies:
            copy.start()
        return copies

    first_row = me * rows
    low_mask = pattern[0, first_row].astype(F32)
    masks = [low_mask] + [pattern[2, first_row + i].astype(F32) for i in range(rows)]
    mu = potential[0]

    def strips():
        return [(r0, slice(r0, r0 + STRIP)) for r0 in range(0, edge_size, STRIP)]

    def unit(r0):
        r = lax.broadcasted_iota(jnp.int32, (STRIP, edge_size), 0) + r0
        c = lax.broadcasted_iota(jnp.int32, (STRIP, edge_size), 1)
        return r == c

    def put(dst, i, slot, strip, x):
        hi, lo = dst
        top = x.astype(BF16)
        hi[i + 1, slot, strip, :] = top
        lo[i + 1, slot, strip, :] = (x - top.astype(F32)).astype(BF16)

    def flipped(x):
        half = edge_size // 2
        top = jnp.concatenate([x[:half, :half].T, x[half:, :half].T], axis=1)
        low = jnp.concatenate([x[:half, half:].T, x[half:, half:].T], axis=1)
        return jnp.concatenate([top, low], axis=0)

    def product(terms):
        total = None
        for (a, i, s), (b, j, p) in terms:
            for left, right in ((0, 0), (1, 0), (0, 1)):
                one = jnp.dot(
                    a[left][i + 1, s], b[right][j + 1, p], preferred_element_type=F32
                )
                total = one if total is None else total + one
        return total

    def band(a, b, i, slot):
        return [
            ((a, i, s), (b, i + s - 1, slot - s + 1))
            for s in range(3)
            if 0 <= slot - s + 1 < 3
        ]

    c, s, d, t = (c_hi, c_lo), (s_hi, s_lo), (d_hi, d_lo), (t_hi, t_lo)

    def put_diagonal(i, source):
        for r0, strip in strips():
            x = jnp.where(unit(r0), mu, 0.0) - source[strip, :]
            put(c, i, 1, strip, x)

    def load_row(i):
        loads[i].wait()

    def split_row(i):
        put_diagonal(i, h.at[i, 1])
        for r0, strip in strips():
            put(c, i, 0, strip, h[i, 0, strip, :] * -masks[i])
            put(c, i, 2, strip, h[i, 2, strip, :] * -masks[i + 1])

    def mirror(i, slot, j, new_slot, mask):
        x = flipped(h[i, slot] * -mask)
        for r0, strip in strips():
            put(c, j, new_slot, strip, x[strip])

    def take_diagonal(dst, k, side, i):
        for r0, strip in strips():
            put(dst, i, 1, strip, halo[k, side, strip, :])

    def square_diagonal(dst, i, x, copy=None):
        for r0, strip in strips():
            y = jnp.where(unit(r0), 3.0, 0.0) - x[strip]
            put(dst, i, 1, strip, y)
            if copy is not None:
                copy[strip, :] = y

    def scaled(dst, i, slot, x, factor, copy=None):
        for r0, strip in strips():
            y = x[strip] * factor
            put(dst, i, slot, strip, y)
            if copy is not None:
                copy[strip, :] = y

    def symmetric_edge(i):
        x = product([((c, i, 1), (c, i, 2)), ((c, i, 2), (c, i + 1, 1))])
        x = x * -masks[i + 1]
        y = flipped(x)
        for r0, strip in strips():
            put(s, i, 2, strip, x[strip])
            put(s, i + 1, 0, strip, y[strip])

    load_row(0)
    load_row(last)
    sent = exchange(0, h.at[0, 1], h.at[last, 1])
    split_row(0)
    split_row(last)
    mirror(0, 0, -1, 2, masks[0])
    mirror(last, 2, rows, 0, masks[rows])
    load_row(1)
    load_row(last - 1)
    split_row(1)
    split_row(last - 1)
    for i in (0, last):
        side = 0 if i == 0 else 1
        square_diagonal(s, i, product(band(c, c, i, 1)), edge.at[0, side])
    sent += exchange(1, edge.at[0, 0], edge.at[0, 1])
    for i in range(2, last - 1):
        load_row(i)
    for i in range(2, last - 1):
        split_row(i)
    for i in range(1, last):
        square_diagonal(s, i, product(band(c, c, i, 1)))
    for i in range(last):
        symmetric_edge(i)
    for copy in sent[0:2]:
        copy.wait_recv()
    hear(0)
    tell(1)
    put_diagonal(-1, halo.at[0, 0])
    put_diagonal(rows, halo.at[0, 1])
    symmetric_edge(-1)
    symmetric_edge(last)

    for i in (0, last):
        side = 0 if i == 0 else 1
        scaled(d, i, 1, product(band(c, s, i, 1)), 0.5, edge.at[1, side])
    sent += exchange(2, edge.at[1, 0], edge.at[1, 1])
    half_masks = [0.5 * m for m in masks]
    for i in range(rows):
        if 0 < i < last:
            scaled(d, i, 1, product(band(c, s, i, 1)), 0.5)
        if i > 0:
            scaled(d, i, 0, product(band(c, s, i, 0)), half_masks[i])
        if i < last:
            scaled(d, i, 2, product(band(c, s, i, 2)), half_masks[i + 1])
    x = product([((c, -1, 1), (s, -1, 2)), ((c, -1, 2), (s, 0, 1))])
    scaled(d, -1, 2, x, half_masks[0])
    x = product([((c, rows, 1), (s, rows, 0)), ((c, rows, 0), (s, last, 1))])
    scaled(d, rows, 0, x, half_masks[rows])
    for copy in sent[2:4]:
        copy.wait_recv()
    hear(1)
    tell(2)
    take_diagonal(s, 1, 0, -1)
    take_diagonal(s, 1, 1, rows)
    scaled(d, 0, 0, product(band(c, s, 0, 0)), half_masks[0])
    scaled(d, last, 2, product(band(c, s, last, 2)), half_masks[rows])

    trace = jnp.zeros((8, edge_size), F32)

    def last_diagonal(i, trace, copy=None):
        own = product([((d, i, 1), (d, i, 1))])
        side = product([((d, i, 0), (d, i - 1, 2)), ((d, i, 2), (d, i + 1, 0))])
        for r0, strip in strips():
            y = jnp.where(unit(r0), 3.0, 0.0) - own[strip]
            z = side[strip]
            put(t, i, 1, strip, y - z)
            if copy is not None:
                copy[strip, :] = y - z
            a = d_hi[i + 1, 1, strip, :].astype(F32) + d_lo[i + 1, 1, strip, :].astype(F32)
            w = a * (y - 3.0 * z)
            for q in range(0, STRIP, 8):
                trace = trace + w[q : q + 8]
        return trace

    trace = last_diagonal(0, trace, edge.at[2, 0])
    trace = last_diagonal(last, trace, edge.at[2, 1])
    sent += exchange(3, edge.at[2, 0], edge.at[2, 1])
    for i in range(1, last):
        trace = last_diagonal(i, trace)
    trace = 0.5 * jnp.sum(trace, axis=0, keepdims=True)
    part[...] = trace[:, :128] + trace[:, 128:]
    pair = pltpu.make_async_remote_copy(
        src_ref=part,
        dst_ref=mate,
        send_sem=trace_send.at[0],
        recv_sem=trace_recv.at[0],
        device_id={"grow": mate_id},
        device_id_type=MESH,
    )
    pair.start()
    minus = [-m for m in masks]
    for i in range(2):
        scaled(t, i, 2, product(band(d, d, i, 2)), minus[i + 1])
    pair.wait()
    hear(2)
    slots[chip] = part[...] + mate[...]
    for k in range(1, n_chips):
        pltpu.make_async_remote_copy(
            src_ref=slots.at[chip],
            dst_ref=slots.at[chip],
            send_sem=trace_send.at[1],
            recv_sem=trace_recv.at[1],
            device_id=at(2 * k),
            device_id_type=MESH,
        ).start()
    for i in range(rows):
        if i > 0:
            scaled(t, i, 0, product(band(d, d, i, 0)), minus[i])
        if 1 < i < last:
            scaled(t, i, 2, product(band(d, d, i, 2)), minus[i + 1])
    for copy in sent[4:6]:
        copy.wait_recv()
    take_diagonal(d, 2, 0, -1)
    take_diagonal(d, 2, 1, rows)
    scaled(t, 0, 0, product(band(d, d, 0, 0)), minus[0])
    scaled(t, last, 2, product(band(d, d, last, 2)), minus[rows])
    x = product([((d, -1, 1), (d, -1, 2)), ((d, -1, 2), (d, 0, 1))])
    scaled(t, -1, 2, x, minus[0])
    x = product([((d, rows, 1), (d, rows, 0)), ((d, rows, 0), (d, last, 1))])
    scaled(t, rows, 0, x, minus[rows])

    def finish(i, slot):
        factor = 0.5 if slot == 1 else half_masks[i + slot // 2]
        out[i, slot] = product(band(d, t, i, slot)) * factor

    for i in range(rows):
        for slot in range(3):
            if (i, slot) not in ((0, 0), (last, 2)):
                finish(i, slot)
    for copy in sent[6:8]:
        copy.wait_recv()
    take_diagonal(t, 3, 0, -1)
    take_diagonal(t, 3, 1, rows)
    finish(0, 0)
    finish(last, 2)

    for copy in sent:
        copy.wait_send()
    others = slots.at[pl.ds(0, n_chips - 1)]
    for sem in (trace_send.at[1], trace_recv.at[1]):
        pltpu.make_async_copy(others, others, sem).wait()
    order = float(rows * n_grow * edge_size)
    occupation[0] = (order + jnp.sum(slots[...])) / (2.0 * order)


def local(n_grow, hamiltonian, pattern, potential):
    rows, slot_count, edge_size, _ = hamiltonian.shape
    full = (rows + 2, slot_count, edge_size, edge_size)
    block = (edge_size, edge_size)
    splits = [pltpu.VMEM(full, BF16) for _ in range(8)]
    steps = max(1, (n_grow // 2).bit_length())
    return pl.pallas_call(
        functools.partial(kernel, n_grow),
        out_shape=(
            pltpu.VMEM(hamiltonian.shape, F32),
            jax.ShapeDtypeStruct((1,), F32),
        ),
        in_specs=[
            pl.BlockSpec(memory_space=pltpu.SMEM),
            pl.BlockSpec(memory_space=pltpu.SMEM),
            pl.BlockSpec(memory_space=pltpu.HBM),
        ],
        out_specs=(
            pl.BlockSpec(memory_space=pltpu.VMEM),
            pl.BlockSpec(memory_space=pltpu.SMEM),
        ),
        scratch_shapes=[
            pltpu.VMEM(hamiltonian.shape, F32),
            *splits,
            pltpu.VMEM((4, 2, *block), F32),
            pltpu.VMEM((3, 2, *block), F32),
            pltpu.VMEM((1, 128), F32),
            pltpu.VMEM((1, 128), F32),
            pltpu.VMEM((n_grow // 2, 1, 128), F32),
            pltpu.SemaphoreType.DMA((rows,)),
            pltpu.SemaphoreType.DMA((4, 2)),
            pltpu.SemaphoreType.DMA((4, 2)),
            pltpu.SemaphoreType.DMA((2,)),
            pltpu.SemaphoreType.DMA((2,)),
            pltpu.SemaphoreType.REGULAR((steps,)),
        ],
        compiler_params=pltpu.CompilerParams(
            collective_id=0,
            has_side_effects=True,
            vmem_limit_bytes=50 * 1024 * 1024,
        ),
        cost_estimate=pl.CostEstimate(
            flops=2 * 166 * 3 * edge_size**3,
            bytes_accessed=2 * 4 * rows * slot_count * edge_size**2,
            transcendentals=0,
        ),
    )(pattern.T, potential, hamiltonian)


def solution(mesh):
    in_specs = (P(("reps", "grow"), None, None, None), P(), P("reps"))
    out_specs = (P(("reps", "grow"), None, None, None), P("reps"))
    step = functools.partial(local, mesh.shape["grow"])

    def run(hamiltonian, pattern, potential):
        return step(hamiltonian, pattern, potential)

    return jax.shard_map(run, mesh=mesh, in_specs=in_specs, out_specs=out_specs, check_vma=False)
```

```python
import functools

import jax
import jax.numpy as jnp
from jax import lax
from jax.experimental import pallas as pl
from jax.experimental.pallas import tpu as pltpu
from jax.sharding import PartitionSpec as P

MESH = pl.DeviceIdType.MESH
F32 = jnp.float32
BF16 = jnp.bfloat16
STRIP = 32


def kernel(
    n_grow,
    pattern_hbm,
    potential,
    h_hbm,
    out,
    occupation,
    pattern,
    h,
    c_hi,
    c_lo,
    s_hi,
    s_lo,
    d_hi,
    d_lo,
    t_hi,
    t_lo,
    halo,
    edge,
    part,
    mate,
    slots,
    load_sem,
    send_sem,
    recv_sem,
    trace_send,
    trace_recv,
    known_sem,
):
    rows, edge_size = h.shape[0], h.shape[2]
    n_chips = n_grow // 2
    last = rows - 1
    me = lax.axis_index("grow")
    chip = me // 2
    mate_id = me + 1 - 2 * lax.rem(me, 2)

    def at(distance):
        return {"grow": lax.rem(me + distance + n_grow, n_grow)}

    small = [
        pltpu.make_async_copy(pattern_hbm, pattern, load_sem.at[rows]),
    ]
    loads = {}
    for i in (0, last, 1, last - 1, 2, 3):
        loads[i] = pltpu.make_async_copy(h_hbm.at[i], h.at[i], load_sem.at[i])
        loads[i].start()
        if i == last:
            for copy in small:
                copy.start()
    barrier = pltpu.get_barrier_semaphore()
    near = [sign * d for d in range(1, 9) for sign in (1, -1)]
    for distance in near:
        pl.semaphore_signal(barrier, inc=1, device_id=at(distance), device_id_type=MESH)
    reaches = []
    reach = 4
    while reach < n_chips // 2:
        reaches.append(reach)
        reach *= 2

    def tell(step):
        if step >= len(reaches):
            return
        for distance in (2 * reaches[step], -2 * reaches[step]):
            pl.semaphore_signal(
                known_sem.at[step], inc=1, device_id=at(distance), device_id_type=MESH
            )

    def hear(step):
        if step >= len(reaches):
            return
        pl.semaphore_wait(known_sem.at[step], 2)

    half = edge_size // 2
    whole = [(slice(0, edge_size), slice(0, edge_size))]
    upper = [(slice(0, half), slice(0, edge_size)), (slice(half, edge_size),) * 2]

    def exchange(k, first, second, pieces):
        copies = []
        for n, (r, c) in enumerate(pieces):
            for side, source, distance in ((1, first, -1), (0, second, 1)):
                copies.append(
                    pltpu.make_async_remote_copy(
                        src_ref=source.at[r, c],
                        dst_ref=halo.at[k, side, r, c],
                        send_sem=send_sem.at[k, side, n],
                        recv_sem=recv_sem.at[k, side, n],
                        device_id=at(distance),
                        device_id_type=MESH,
                    )
                )
        for copy in copies:
            copy.start()
        return copies

    def arrived(copies, k, pieces):
        for copy in copies:
            copy.wait_recv()
        if pieces is upper:
            for side in range(2):
                block = halo.at[k, side]
                block[half:, :half] = block[:half, half:].T

    first_row = me * rows
    for copy in small:
        copy.wait()
    low_mask = pattern[0, first_row].astype(F32)
    masks = [low_mask] + [pattern[2, first_row + i].astype(F32) for i in range(rows)]
    mu = potential[0]

    def strips():
        return [(r0, slice(r0, r0 + STRIP)) for r0 in range(0, edge_size, STRIP)]

    def unit(r0):
        r = lax.broadcasted_iota(jnp.int32, (STRIP, edge_size), 0) + r0
        c = lax.broadcasted_iota(jnp.int32, (STRIP, edge_size), 1)
        return r == c

    def put(dst, i, slot, strip, x):
        hi, lo = dst
        top = x.astype(BF16)
        hi[i + 1, slot, strip, :] = top
        lo[i + 1, slot, strip, :] = (x - top.astype(F32)).astype(BF16)

    def flipped(x):
        top = jnp.concatenate([x[:half, :half].T, x[half:, :half].T], axis=1)
        low = jnp.concatenate([x[:half, half:].T, x[half:, half:].T], axis=1)
        return jnp.concatenate([top, low], axis=0)

    def product(terms):
        total = None
        for (a, i, s), (b, j, p) in terms:
            for left, right in ((0, 0), (1, 0), (0, 1)):
                one = jnp.dot(
                    a[left][i + 1, s], b[right][j + 1, p], preferred_element_type=F32
                )
                total = one if total is None else total + one
        return total

    def band(a, b, i, slot):
        return [
            ((a, i, s), (b, i + s - 1, slot - s + 1))
            for s in range(3)
            if 0 <= slot - s + 1 < 3
        ]

    c, s, d, t = (c_hi, c_lo), (s_hi, s_lo), (d_hi, d_lo), (t_hi, t_lo)

    def put_diagonal(i, source):
        for r0, strip in strips():
            x = jnp.where(unit(r0), mu, 0.0) - source[strip, :]
            put(c, i, 1, strip, x)

    def load_row(i):
        loads[i].wait()

    def split(i, slot):
        if slot == 1:
            put_diagonal(i, h.at[i, 1])
        else:
            for r0, strip in strips():
                put(c, i, slot, strip, h[i, slot, strip, :] * -masks[i + slot // 2])

    def split_row(i):
        for slot in range(3):
            split(i, slot)

    def mirror(i, slot, j, new_slot, mask):
        x = flipped(h[i, slot] * -mask)
        for r0, strip in strips():
            put(c, j, new_slot, strip, x[strip])

    def take_diagonal(dst, k, side, i):
        for r0, strip in strips():
            put(dst, i, 1, strip, halo[k, side, strip, :])

    def square_diagonal(dst, i, x, copy=None):
        for r0, strip in strips():
            y = jnp.where(unit(r0), 3.0, 0.0) - x[strip]
            put(dst, i, 1, strip, y)
            if copy is not None:
                copy[strip, :] = y

    def scaled(dst, i, slot, x, factor, copy=None):
        for r0, strip in strips():
            y = x[strip] * factor
            put(dst, i, slot, strip, y)
            if copy is not None:
                copy[strip, :] = y

    def symmetric_edge(i):
        x = product([((c, i, 1), (c, i, 2)), ((c, i, 2), (c, i + 1, 1))])
        x = x * -masks[i + 1]
        y = flipped(x)
        for r0, strip in strips():
            put(s, i, 2, strip, x[strip])
            put(s, i + 1, 0, strip, y[strip])

    load_row(0)
    load_row(last)
    split_row(0)
    split_row(last)
    mirror(0, 0, -1, 2, masks[0])
    mirror(last, 2, rows, 0, masks[rows])
    load_row(1)
    load_row(last - 1)
    for i in (1, last - 1):
        split_row(i)
    for i in (0, last):
        side = 0 if i == 0 else 1
        square_diagonal(s, i, product(band(c, c, i, 1)), edge.at[0, side])
    symmetric_edge(0)
    symmetric_edge(last - 1)
    pl.semaphore_wait(barrier, len(near))
    tell(0)
    sent0 = exchange(0, h.at[0, 1], h.at[last, 1], upper)
    sent1 = exchange(1, edge.at[0, 0], edge.at[0, 1], upper)
    for i in range(2, last - 1):
        load_row(i)

    half_masks = [0.5 * m for m in masks]

    def step(i, slot, copy=None):
        factor = 0.5 if slot == 1 else half_masks[i + slot // 2]
        scaled(d, i, slot, product(band(c, s, i, slot)), factor, copy)

    for i in range(2, last - 1):
        split_row(i)
    for i in range(1, last):
        square_diagonal(s, i, product(band(c, c, i, 1)))
    for i in range(1, last - 1):
        symmetric_edge(i)
    step(0, 2)
    step(1, 0)
    step(1, 1)
    step(1, 2)
    hear(0)
    tell(1)
    for i in range(2, rows):
        for slot in range(3):
            if i < last or slot == 0:
                step(i, slot)
    arrived(sent0, 0, upper)

    put_diagonal(-1, halo.at[0, 0])
    put_diagonal(rows, halo.at[0, 1])
    symmetric_edge(-1)
    symmetric_edge(last)
    step(0, 1, edge.at[1, 0])
    step(last, 1, edge.at[1, 1])
    x = product([((c, -1, 1), (s, -1, 2)), ((c, -1, 2), (s, 0, 1))])
    scaled(d, -1, 2, x, half_masks[0])
    x = product([((c, rows, 1), (s, rows, 0)), ((c, rows, 0), (s, last, 1))])
    scaled(d, rows, 0, x, half_masks[rows])
    sent2 = exchange(2, edge.at[1, 0], edge.at[1, 1], upper)
    arrived(sent1, 1, upper)
    take_diagonal(s, 1, 0, -1)
    take_diagonal(s, 1, 1, rows)
    step(0, 0)
    step(last, 2)

    trace = jnp.zeros((8, edge_size), F32)

    def last_diagonal(i, trace, copy=None):
        own = product([((d, i, 1), (d, i, 1))])
        side = product([((d, i, 0), (d, i - 1, 2)), ((d, i, 2), (d, i + 1, 0))])
        for r0, strip in strips():
            y = jnp.where(unit(r0), 3.0, 0.0) - own[strip]
            z = side[strip]
            put(t, i, 1, strip, y - z)
            if copy is not None:
                copy[strip, :] = y - z
            a = d_hi[i + 1, 1, strip, :].astype(F32) + d_lo[i + 1, 1, strip, :].astype(F32)
            w = a * (y - 3.0 * z)
            for q in range(0, STRIP, 8):
                trace = trace + w[q : q + 8]
        return trace

    for i in range(1, last):
        trace = last_diagonal(i, trace)
    trace = last_diagonal(0, trace, edge.at[2, 0])
    trace = last_diagonal(last, trace, edge.at[2, 1])
    trace = 0.5 * jnp.sum(trace, axis=0, keepdims=True)
    part[...] = trace[:, :128] + trace[:, 128:]
    minus = [-m for m in masks]

    def inner(i, slot):
        scaled(t, i, slot, product(band(d, d, i, slot)), minus[i + slot // 2])

    inside = [(i, slot) for i in range(rows) for slot in (0, 2) if 0 <= i + slot - 1 < rows]
    hear(1)
    slots[me] = part[...]
    for k in sorted(range(1, n_grow), key=lambda k: -min(k, n_grow - k)):
        pltpu.make_async_remote_copy(
            src_ref=slots.at[me],
            dst_ref=slots.at[me],
            send_sem=trace_send.at[1],
            recv_sem=trace_recv.at[1],
            device_id=at(k),
            device_id_type=MESH,
        ).start()
    sent3 = exchange(3, edge.at[2, 0], edge.at[2, 1], whole)
    for i, slot in inside:
        inner(i, slot)

    def finish(i, slot):
        factor = 0.5 if slot == 1 else half_masks[i + slot // 2]
        out[i, slot] = product(band(d, t, i, slot)) * factor

    for i in range(rows):
        for slot in range(3):
            if 0 < i < last or (i, slot) in ((0, 2), (last, 0)):
                finish(i, slot)
    arrived(sent2, 2, upper)
    take_diagonal(d, 2, 0, -1)
    take_diagonal(d, 2, 1, rows)
    x = product([((d, -1, 1), (d, -1, 2)), ((d, -1, 2), (d, 0, 1))])
    scaled(t, -1, 2, x, minus[0])
    x = product([((d, rows, 1), (d, rows, 0)), ((d, rows, 0), (d, last, 1))])
    scaled(t, rows, 0, x, minus[rows])
    scaled(t, 0, 0, product(band(d, d, 0, 0)), minus[0])
    scaled(t, last, 2, product(band(d, d, last, 2)), minus[rows])
    finish(0, 1)
    finish(last, 1)
    arrived(sent3, 3, whole)
    take_diagonal(t, 3, 0, -1)
    take_diagonal(t, 3, 1, rows)
    finish(0, 0)
    finish(last, 2)

    for copy in sent0 + sent1 + sent2 + sent3:
        copy.wait_send()
    others = slots.at[pl.ds(0, n_grow - 1)]
    for sem in (trace_send.at[1], trace_recv.at[1]):
        pltpu.make_async_copy(others, others, sem).wait()
    order = float(rows * n_grow * edge_size)
    occupation[0] = (order + jnp.sum(slots[...])) / (2.0 * order)


def local(n_grow, hamiltonian, pattern, potential):
    rows, slot_count, edge_size, _ = hamiltonian.shape
    full = (rows + 2, slot_count, edge_size, edge_size)
    block = (edge_size, edge_size)
    splits = [pltpu.VMEM(full, BF16) for _ in range(8)]
    steps = max(1, (n_grow // 2).bit_length())
    return pl.pallas_call(
        functools.partial(kernel, n_grow),
        out_shape=(
            pltpu.VMEM(hamiltonian.shape, F32),
            jax.ShapeDtypeStruct((1,), F32),
        ),
        in_specs=[
            pl.BlockSpec(memory_space=pltpu.HBM),
            pl.BlockSpec(memory_space=pltpu.SMEM),
            pl.BlockSpec(memory_space=pltpu.HBM),
        ],
        out_specs=(
            pl.BlockSpec(memory_space=pltpu.VMEM),
            pl.BlockSpec(memory_space=pltpu.SMEM),
        ),
        scratch_shapes=[
            pltpu.SMEM(pattern.shape[::-1], jnp.int32),
            pltpu.VMEM(hamiltonian.shape, F32),
            *splits,
            pltpu.VMEM((4, 2, *block), F32),
            pltpu.VMEM((3, 2, *block), F32),
            pltpu.VMEM((1, 128), F32),
            pltpu.VMEM((1, 128), F32),
            pltpu.VMEM((n_grow, 1, 128), F32),
            pltpu.SemaphoreType.DMA((rows + 1,)),
            pltpu.SemaphoreType.DMA((4, 2, 2)),
            pltpu.SemaphoreType.DMA((4, 2, 2)),
            pltpu.SemaphoreType.DMA((2,)),
            pltpu.SemaphoreType.DMA((2,)),
            pltpu.SemaphoreType.REGULAR((steps,)),
        ],
        compiler_params=pltpu.CompilerParams(
            collective_id=0,
            has_side_effects=True,
            vmem_limit_bytes=50 * 1024 * 1024,
        ),
        cost_estimate=pl.CostEstimate(
            flops=2 * 166 * 3 * edge_size**3,
            bytes_accessed=2 * 4 * rows * slot_count * edge_size**2,
            transcendentals=0,
        ),
    )(pattern.T, potential, hamiltonian)


def solution(mesh):
    in_specs = (P(("reps", "grow"), None, None, None), P(), P("reps"))
    out_specs = (P(("reps", "grow"), None, None, None), P("reps"))
    step = functools.partial(local, mesh.shape["grow"])

    def run(hamiltonian, pattern, potential):
        return step(hamiltonian, pattern, potential)

    return jax.shard_map(run, mesh=mesh, in_specs=in_specs, out_specs=out_specs, check_vma=False)
```

```python
import functools

import jax
import jax.numpy as jnp
from jax import lax
from jax.experimental import pallas as pl
from jax.experimental.pallas import tpu as pltpu
from jax.sharding import PartitionSpec as P

MESH = pl.DeviceIdType.MESH
F32 = jnp.float32
BF16 = jnp.bfloat16
STRIP = 32


def kernel(
    n_grow,
    pattern_hbm,
    potential,
    h_hbm,
    out,
    occupation,
    pattern,
    h,
    c_hi,
    c_lo,
    s_hi,
    s_lo,
    d_hi,
    d_lo,
    t_hi,
    t_lo,
    halo,
    edge,
    part,
    mate,
    slots,
    load_sem,
    send_sem,
    recv_sem,
    trace_send,
    trace_recv,
    known_sem,
):
    rows, edge_size = h.shape[0], h.shape[2]
    n_chips = n_grow // 2
    last = rows - 1
    me = lax.axis_index("grow")
    chip = me // 2
    mate_id = me + 1 - 2 * lax.rem(me, 2)

    def at(distance):
        return {"grow": lax.rem(me + distance + n_grow, n_grow)}

    small = [
        pltpu.make_async_copy(pattern_hbm, pattern, load_sem.at[rows]),
    ]
    loads = {}
    for i in (0, last, 1, last - 1, 2, 3):
        loads[i] = pltpu.make_async_copy(h_hbm.at[i], h.at[i], load_sem.at[i])
        loads[i].start()
        if i == last:
            for copy in small:
                copy.start()
    barrier = pltpu.get_barrier_semaphore()
    near = [sign * d for d in range(1, 9) for sign in (1, -1)]
    for distance in near:
        pl.semaphore_signal(barrier, inc=1, device_id=at(distance), device_id_type=MESH)
    reaches = []
    reach = 4
    while reach < n_chips // 2:
        reaches.append(reach)
        reach *= 2

    def tell(step):
        if step >= len(reaches):
            return
        for distance in (2 * reaches[step], -2 * reaches[step]):
            pl.semaphore_signal(
                known_sem.at[step], inc=1, device_id=at(distance), device_id_type=MESH
            )

    def hear(step):
        if step >= len(reaches):
            return
        pl.semaphore_wait(known_sem.at[step], 2)

    half = edge_size // 2
    whole = [(slice(0, edge_size), slice(0, edge_size))]
    upper = [(slice(0, half), slice(0, edge_size)), (slice(half, edge_size),) * 2]

    def exchange(k, first, second, pieces):
        copies = []
        for n, (r, c) in enumerate(pieces):
            for side, source, distance in ((1, first, -1), (0, second, 1)):
                copies.append(
                    pltpu.make_async_remote_copy(
                        src_ref=source.at[r, c],
                        dst_ref=halo.at[k, side, r, c],
                        send_sem=send_sem.at[k, side, n],
                        recv_sem=recv_sem.at[k, side, n],
                        device_id=at(distance),
                        device_id_type=MESH,
                    )
                )
        for copy in copies:
            copy.start()
        return copies

    def arrived(copies, k, pieces):
        for copy in copies:
            copy.wait_recv()
        if pieces is upper:
            for side in range(2):
                block = halo.at[k, side]
                block[half:, :half] = block[:half, half:].T

    first_row = me * rows
    for copy in small:
        copy.wait()
    low_mask = pattern[0, first_row].astype(F32)
    masks = [low_mask] + [pattern[2, first_row + i].astype(F32) for i in range(rows)]
    mu = potential[0]

    def strips():
        return [(r0, slice(r0, r0 + STRIP)) for r0 in range(0, edge_size, STRIP)]

    def unit(r0):
        r = lax.broadcasted_iota(jnp.int32, (STRIP, edge_size), 0) + r0
        c = lax.broadcasted_iota(jnp.int32, (STRIP, edge_size), 1)
        return r == c

    def put(dst, i, slot, strip, x):
        hi, lo = dst
        top = x.astype(BF16)
        hi[i + 1, slot, strip, :] = top
        lo[i + 1, slot, strip, :] = (x - top.astype(F32)).astype(BF16)

    def flipped(x):
        top = jnp.concatenate([x[:half, :half].T, x[half:, :half].T], axis=1)
        low = jnp.concatenate([x[:half, half:].T, x[half:, half:].T], axis=1)
        return jnp.concatenate([top, low], axis=0)

    def product(terms):
        total = None
        for (a, i, s), (b, j, p) in terms:
            for left, right in ((0, 0), (1, 0), (0, 1)):
                one = jnp.dot(
                    a[left][i + 1, s], b[right][j + 1, p], preferred_element_type=F32
                )
                total = one if total is None else total + one
        return total

    def band(a, b, i, slot):
        return [
            ((a, i, s), (b, i + s - 1, slot - s + 1))
            for s in range(3)
            if 0 <= slot - s + 1 < 3
        ]

    c, s, d, t = (c_hi, c_lo), (s_hi, s_lo), (d_hi, d_lo), (t_hi, t_lo)

    def put_diagonal(i, source):
        for r0, strip in strips():
            x = jnp.where(unit(r0), mu, 0.0) - source[strip, :]
            put(c, i, 1, strip, x)

    def load_row(i):
        loads[i].wait()

    def split(i, slot):
        if slot == 1:
            put_diagonal(i, h.at[i, 1])
        else:
            for r0, strip in strips():
                put(c, i, slot, strip, h[i, slot, strip, :] * -masks[i + slot // 2])

    def split_row(i):
        for slot in range(3):
            split(i, slot)

    def mirror(i, slot, j, new_slot, mask):
        x = flipped(h[i, slot] * -mask)
        for r0, strip in strips():
            put(c, j, new_slot, strip, x[strip])

    def take_diagonal(dst, k, side, i):
        for r0, strip in strips():
            put(dst, i, 1, strip, halo[k, side, strip, :])

    def square_diagonal(dst, i, x, copy=None):
        for r0, strip in strips():
            y = jnp.where(unit(r0), 3.0, 0.0) - x[strip]
            put(dst, i, 1, strip, y)
            if copy is not None:
                copy[strip, :] = y

    def scaled(dst, i, slot, x, factor, copy=None):
        for r0, strip in strips():
            y = x[strip] * factor
            put(dst, i, slot, strip, y)
            if copy is not None:
                copy[strip, :] = y

    def symmetric_edge(i):
        x = product([((c, i, 1), (c, i, 2)), ((c, i, 2), (c, i + 1, 1))])
        x = x * -masks[i + 1]
        y = flipped(x)
        for r0, strip in strips():
            put(s, i, 2, strip, x[strip])
            put(s, i + 1, 0, strip, y[strip])

    for i in (0, last, 1, last - 1):
        load_row(i)
    split_row(0)
    split_row(last)
    mirror(0, 0, -1, 2, masks[0])
    mirror(last, 2, rows, 0, masks[rows])
    for i in (1, last - 1):
        split_row(i)
    for i in (0, last):
        side = 0 if i == 0 else 1
        square_diagonal(s, i, product(band(c, c, i, 1)), edge.at[0, side])
    symmetric_edge(0)
    symmetric_edge(last - 1)
    pl.semaphore_wait(barrier, len(near))
    tell(0)
    sent0 = exchange(0, h.at[0, 1], h.at[last, 1], upper)
    sent1 = exchange(1, edge.at[0, 0], edge.at[0, 1], upper)
    for i in range(2, last - 1):
        load_row(i)

    half_masks = [0.5 * m for m in masks]

    def step(i, slot, copy=None):
        factor = 0.5 if slot == 1 else half_masks[i + slot // 2]
        scaled(d, i, slot, product(band(c, s, i, slot)), factor, copy)

    for i in range(2, last - 1):
        split_row(i)
    for i in range(1, last):
        square_diagonal(s, i, product(band(c, c, i, 1)))
    for i in range(1, last - 1):
        symmetric_edge(i)
    step(0, 2)
    step(1, 0)
    step(1, 1)
    step(1, 2)
    hear(0)
    tell(1)
    for i in range(2, rows):
        for slot in range(3):
            if i < last or slot == 0:
                step(i, slot)
    arrived(sent0, 0, upper)

    put_diagonal(-1, halo.at[0, 0])
    put_diagonal(rows, halo.at[0, 1])
    symmetric_edge(-1)
    symmetric_edge(last)
    step(0, 1, edge.at[1, 0])
    step(last, 1, edge.at[1, 1])
    x = product([((c, -1, 1), (s, -1, 2)), ((c, -1, 2), (s, 0, 1))])
    scaled(d, -1, 2, x, half_masks[0])
    x = product([((c, rows, 1), (s, rows, 0)), ((c, rows, 0), (s, last, 1))])
    scaled(d, rows, 0, x, half_masks[rows])
    sent2 = exchange(2, edge.at[1, 0], edge.at[1, 1], upper)
    arrived(sent1, 1, upper)
    take_diagonal(s, 1, 0, -1)
    take_diagonal(s, 1, 1, rows)
    step(0, 0)
    step(last, 2)

    trace = jnp.zeros((8, edge_size), F32)

    def last_diagonal(i, trace, copy=None):
        own = product([((d, i, 1), (d, i, 1))])
        side = product([((d, i, 0), (d, i - 1, 2)), ((d, i, 2), (d, i + 1, 0))])
        for r0, strip in strips():
            y = jnp.where(unit(r0), 3.0, 0.0) - own[strip]
            z = side[strip]
            put(t, i, 1, strip, y - z)
            if copy is not None:
                copy[strip, :] = y - z
            a = d_hi[i + 1, 1, strip, :].astype(F32) + d_lo[i + 1, 1, strip, :].astype(F32)
            w = a * (y - 3.0 * z)
            for q in range(0, STRIP, 8):
                trace = trace + w[q : q + 8]
        return trace

    for i in range(1, last):
        trace = last_diagonal(i, trace)
    trace = last_diagonal(0, trace, edge.at[2, 0])
    trace = last_diagonal(last, trace, edge.at[2, 1])
    trace = 0.5 * jnp.sum(trace, axis=0, keepdims=True)
    part[...] = trace[:, :128] + trace[:, 128:]
    minus = [-m for m in masks]

    def inner(i, slot):
        scaled(t, i, slot, product(band(d, d, i, slot)), minus[i + slot // 2])

    inside = [(i, slot) for i in range(rows) for slot in (0, 2) if 0 <= i + slot - 1 < rows]
    hear(1)
    slots[me] = part[...]
    for k in sorted(range(1, n_grow), key=lambda k: -min(k, n_grow - k)):
        pltpu.make_async_remote_copy(
            src_ref=slots.at[me],
            dst_ref=slots.at[me],
            send_sem=trace_send.at[1],
            recv_sem=trace_recv.at[1],
            device_id=at(k),
            device_id_type=MESH,
        ).start()
    sent3 = exchange(3, edge.at[2, 0], edge.at[2, 1], whole)
    for i, slot in inside:
        inner(i, slot)

    def finish(i, slot):
        factor = 0.5 if slot == 1 else half_masks[i + slot // 2]
        out[i, slot] = product(band(d, t, i, slot)) * factor

    for i in range(rows):
        for slot in range(3):
            if 0 < i < last or (i, slot) in ((0, 2), (last, 0)):
                finish(i, slot)
    arrived(sent2, 2, upper)
    take_diagonal(d, 2, 0, -1)
    take_diagonal(d, 2, 1, rows)
    x = product([((d, -1, 1), (d, -1, 2)), ((d, -1, 2), (d, 0, 1))])
    scaled(t, -1, 2, x, minus[0])
    x = product([((d, rows, 1), (d, rows, 0)), ((d, rows, 0), (d, last, 1))])
    scaled(t, rows, 0, x, minus[rows])
    scaled(t, 0, 0, product(band(d, d, 0, 0)), minus[0])
    scaled(t, last, 2, product(band(d, d, last, 2)), minus[rows])
    finish(0, 1)
    finish(last, 1)
    arrived(sent3, 3, whole)
    take_diagonal(t, 3, 0, -1)
    take_diagonal(t, 3, 1, rows)
    finish(0, 0)
    finish(last, 2)

    for copy in sent0 + sent1 + sent2 + sent3:
        copy.wait_send()
    others = slots.at[pl.ds(0, n_grow - 1)]
    for sem in (trace_send.at[1], trace_recv.at[1]):
        pltpu.make_async_copy(others, others, sem).wait()
    order = float(rows * n_grow * edge_size)
    occupation[0] = (order + jnp.sum(slots[...])) / (2.0 * order)


def local(n_grow, hamiltonian, pattern, potential):
    rows, slot_count, edge_size, _ = hamiltonian.shape
    full = (rows + 2, slot_count, edge_size, edge_size)
    block = (edge_size, edge_size)
    splits = [pltpu.VMEM(full, BF16) for _ in range(8)]
    steps = max(1, (n_grow // 2).bit_length())
    return pl.pallas_call(
        functools.partial(kernel, n_grow),
        out_shape=(
            pltpu.VMEM(hamiltonian.shape, F32),
            pltpu.SMEM((1,), F32),
        ),
        in_specs=[
            pl.BlockSpec(memory_space=pltpu.HBM),
            pl.BlockSpec(memory_space=pltpu.SMEM),
            pl.BlockSpec(memory_space=pltpu.HBM),
        ],
        out_specs=(
            pl.BlockSpec(memory_space=pltpu.VMEM),
            pl.BlockSpec(memory_space=pltpu.SMEM),
        ),
        scratch_shapes=[
            pltpu.SMEM(pattern.shape[::-1], jnp.int32),
            pltpu.VMEM(hamiltonian.shape, F32),
            *splits,
            pltpu.VMEM((4, 2, *block), F32),
            pltpu.VMEM((3, 2, *block), F32),
            pltpu.VMEM((1, 128), F32),
            pltpu.VMEM((1, 128), F32),
            pltpu.VMEM((n_grow, 1, 128), F32),
            pltpu.SemaphoreType.DMA((rows + 1,)),
            pltpu.SemaphoreType.DMA((4, 2, 2)),
            pltpu.SemaphoreType.DMA((4, 2, 2)),
            pltpu.SemaphoreType.DMA((2,)),
            pltpu.SemaphoreType.DMA((2,)),
            pltpu.SemaphoreType.REGULAR((steps,)),
        ],
        compiler_params=pltpu.CompilerParams(
            collective_id=0,
            has_side_effects=True,
            vmem_limit_bytes=50 * 1024 * 1024,
        ),
        cost_estimate=pl.CostEstimate(
            flops=2 * 166 * 3 * edge_size**3,
            bytes_accessed=2 * 4 * rows * slot_count * edge_size**2,
            transcendentals=0,
        ),
    )(pattern.T, potential, hamiltonian)


def solution(mesh):
    in_specs = (P(("reps", "grow"), None, None, None), P(), P("reps"))
    out_specs = (P(("reps", "grow"), None, None, None), P("reps"))
    step = functools.partial(local, mesh.shape["grow"])

    def run(hamiltonian, pattern, potential):
        return step(hamiltonian, pattern, potential)

    return jax.shard_map(run, mesh=mesh, in_specs=in_specs, out_specs=out_specs, check_vma=False)
```

```python
import functools

import jax
import jax.numpy as jnp
from jax import lax
from jax.experimental import pallas as pl
from jax.experimental.pallas import tpu as pltpu
from jax.sharding import PartitionSpec as P

MESH = pl.DeviceIdType.MESH
F32 = jnp.float32
BF16 = jnp.bfloat16
STRIP = 32
BEFORE = 5


def kernel(
    n_grow,
    pattern_hbm,
    potential,
    h_hbm,
    out,
    occupation,
    pattern,
    h,
    c_hi,
    c_lo,
    s_hi,
    s_lo,
    d_hi,
    d_lo,
    t_hi,
    t_lo,
    halo,
    edge,
    part,
    mate,
    slots,
    load_sem,
    send_sem,
    recv_sem,
    trace_send,
    trace_recv,
    known_sem,
):
    rows, edge_size = h.shape[0], h.shape[2]
    n_chips = n_grow // 2
    last = rows - 1
    me = lax.axis_index("grow")
    chip = me // 2
    mate_id = me + 1 - 2 * lax.rem(me, 2)

    def at(distance):
        return {"grow": lax.rem(me + distance + n_grow, n_grow)}

    small = [
        pltpu.make_async_copy(pattern_hbm, pattern, load_sem.at[rows]),
    ]
    loads = {}
    for i in (0, last, 1, last - 1, 2, 3):
        loads[i] = pltpu.make_async_copy(h_hbm.at[i], h.at[i], load_sem.at[i])
        loads[i].start()
        if i == last:
            for copy in small:
                copy.start()
    barrier = pltpu.get_barrier_semaphore()
    near = [sign * d for d in range(1, 9) for sign in (1, -1)]
    for distance in near:
        pl.semaphore_signal(barrier, inc=1, device_id=at(distance), device_id_type=MESH)
    reaches = []
    reach = 4
    while reach < n_chips // 2:
        reaches.append(reach)
        reach *= 2

    def tell(step):
        if step >= len(reaches):
            return
        for distance in (2 * reaches[step], -2 * reaches[step]):
            pl.semaphore_signal(
                known_sem.at[step], inc=1, device_id=at(distance), device_id_type=MESH
            )

    def hear(step):
        if step >= len(reaches):
            return
        pl.semaphore_wait(known_sem.at[step], 2)

    half = edge_size // 2
    whole = [(slice(0, edge_size), slice(0, edge_size))]
    upper = [(slice(0, half), slice(0, edge_size)), (slice(half, edge_size),) * 2]

    def exchange(k, first, second, pieces):
        copies = []
        for n, (r, c) in enumerate(pieces):
            for side, source, distance in ((1, first, -1), (0, second, 1)):
                copies.append(
                    pltpu.make_async_remote_copy(
                        src_ref=source.at[r, c],
                        dst_ref=halo.at[k, side, r, c],
                        send_sem=send_sem.at[k, side, n],
                        recv_sem=recv_sem.at[k, side, n],
                        device_id=at(distance),
                        device_id_type=MESH,
                    )
                )
        for copy in copies:
            copy.start()
        return copies

    def arrived(copies, k, pieces):
        for copy in copies:
            copy.wait_recv()
        if pieces is upper:
            for side in range(2):
                block = halo.at[k, side]
                block[half:, :half] = block[:half, half:].T

    first_row = me * rows
    for copy in small:
        copy.wait()
    low_mask = pattern[0, first_row].astype(F32)
    masks = [low_mask] + [pattern[2, first_row + i].astype(F32) for i in range(rows)]
    mu = potential[0]

    def strips():
        return [(r0, slice(r0, r0 + STRIP)) for r0 in range(0, edge_size, STRIP)]

    def unit(r0):
        r = lax.broadcasted_iota(jnp.int32, (STRIP, edge_size), 0) + r0
        c = lax.broadcasted_iota(jnp.int32, (STRIP, edge_size), 1)
        return r == c

    def put(dst, i, slot, strip, x):
        hi, lo = dst
        top = x.astype(BF16)
        hi[i + 1, slot, strip, :] = top
        lo[i + 1, slot, strip, :] = (x - top.astype(F32)).astype(BF16)

    def flipped(x):
        top = jnp.concatenate([x[:half, :half].T, x[half:, :half].T], axis=1)
        low = jnp.concatenate([x[:half, half:].T, x[half:, half:].T], axis=1)
        return jnp.concatenate([top, low], axis=0)

    def product(terms):
        total = None
        for (a, i, s), (b, j, p) in terms:
            for left, right in ((0, 0), (1, 0), (0, 1)):
                one = jnp.dot(
                    a[left][i + 1, s], b[right][j + 1, p], preferred_element_type=F32
                )
                total = one if total is None else total + one
        return total

    def band(a, b, i, slot):
        return [
            ((a, i, s), (b, i + s - 1, slot - s + 1))
            for s in range(3)
            if 0 <= slot - s + 1 < 3
        ]

    c, s, d, t = (c_hi, c_lo), (s_hi, s_lo), (d_hi, d_lo), (t_hi, t_lo)

    def put_diagonal(i, source):
        for r0, strip in strips():
            x = jnp.where(unit(r0), mu, 0.0) - source[strip, :]
            put(c, i, 1, strip, x)

    def load_row(i):
        loads[i].wait()

    def split(i, slot):
        if slot == 1:
            put_diagonal(i, h.at[i, 1])
        else:
            for r0, strip in strips():
                put(c, i, slot, strip, h[i, slot, strip, :] * -masks[i + slot // 2])

    def split_row(i):
        for slot in range(3):
            split(i, slot)

    def mirror(i, slot, j, new_slot, mask):
        x = flipped(h[i, slot] * -mask)
        for r0, strip in strips():
            put(c, j, new_slot, strip, x[strip])

    def take_diagonal(dst, k, side, i):
        for r0, strip in strips():
            put(dst, i, 1, strip, halo[k, side, strip, :])

    def square_diagonal(dst, i, x, copy=None):
        for r0, strip in strips():
            y = jnp.where(unit(r0), 3.0, 0.0) - x[strip]
            put(dst, i, 1, strip, y)
            if copy is not None:
                copy[strip, :] = y

    def scaled(dst, i, slot, x, factor, copy=None):
        for r0, strip in strips():
            y = x[strip] * factor
            put(dst, i, slot, strip, y)
            if copy is not None:
                copy[strip, :] = y

    def symmetric_edge(i):
        x = product([((c, i, 1), (c, i, 2)), ((c, i, 2), (c, i + 1, 1))])
        x = x * -masks[i + 1]
        y = flipped(x)
        for r0, strip in strips():
            put(s, i, 2, strip, x[strip])
            put(s, i + 1, 0, strip, y[strip])

    for i in (0, last, 1, last - 1):
        load_row(i)
    split_row(0)
    split_row(last)
    mirror(0, 0, -1, 2, masks[0])
    mirror(last, 2, rows, 0, masks[rows])
    for i in (1, last - 1):
        split_row(i)
    for i in (0, last):
        side = 0 if i == 0 else 1
        square_diagonal(s, i, product(band(c, c, i, 1)), edge.at[0, side])
    symmetric_edge(0)
    symmetric_edge(last - 1)
    pl.semaphore_wait(barrier, len(near))
    tell(0)
    sent0 = exchange(0, h.at[0, 1], h.at[last, 1], upper)
    sent1 = exchange(1, edge.at[0, 0], edge.at[0, 1], upper)
    for i in range(2, last - 1):
        load_row(i)

    half_masks = [0.5 * m for m in masks]

    def step(i, slot, copy=None):
        factor = 0.5 if slot == 1 else half_masks[i + slot // 2]
        scaled(d, i, slot, product(band(c, s, i, slot)), factor, copy)

    for i in range(2, last - 1):
        split_row(i)
    for i in range(1, last):
        square_diagonal(s, i, product(band(c, c, i, 1)))
    for i in range(1, last - 1):
        symmetric_edge(i)
    step(0, 2)
    near_rows = [(i, slot) for i in range(1, rows) for slot in range(3) if i < last or slot == 0]
    for i, slot in near_rows[:BEFORE]:
        step(i, slot)
    hear(0)
    tell(1)
    for i, slot in near_rows[BEFORE:]:
        step(i, slot)
    arrived(sent0, 0, upper)

    put_diagonal(-1, halo.at[0, 0])
    put_diagonal(rows, halo.at[0, 1])
    symmetric_edge(-1)
    symmetric_edge(last)
    step(0, 1, edge.at[1, 0])
    step(last, 1, edge.at[1, 1])
    x = product([((c, -1, 1), (s, -1, 2)), ((c, -1, 2), (s, 0, 1))])
    scaled(d, -1, 2, x, half_masks[0])
    x = product([((c, rows, 1), (s, rows, 0)), ((c, rows, 0), (s, last, 1))])
    scaled(d, rows, 0, x, half_masks[rows])
    sent2 = exchange(2, edge.at[1, 0], edge.at[1, 1], upper)
    arrived(sent1, 1, upper)
    take_diagonal(s, 1, 0, -1)
    take_diagonal(s, 1, 1, rows)
    step(0, 0)
    step(last, 2)

    trace = jnp.zeros((8, edge_size), F32)

    def last_diagonal(i, trace, copy=None):
        own = product([((d, i, 1), (d, i, 1))])
        side = product([((d, i, 0), (d, i - 1, 2)), ((d, i, 2), (d, i + 1, 0))])
        for r0, strip in strips():
            y = jnp.where(unit(r0), 3.0, 0.0) - own[strip]
            z = side[strip]
            put(t, i, 1, strip, y - z)
            if copy is not None:
                copy[strip, :] = y - z
            a = d_hi[i + 1, 1, strip, :].astype(F32) + d_lo[i + 1, 1, strip, :].astype(F32)
            w = a * (y - 3.0 * z)
            for q in range(0, STRIP, 8):
                trace = trace + w[q : q + 8]
        return trace

    for i in range(1, last):
        trace = last_diagonal(i, trace)
    trace = last_diagonal(0, trace, edge.at[2, 0])
    trace = last_diagonal(last, trace, edge.at[2, 1])
    trace = 0.5 * jnp.sum(trace, axis=0, keepdims=True)
    part[...] = trace[:, :128] + trace[:, 128:]
    minus = [-m for m in masks]

    def inner(i, slot):
        scaled(t, i, slot, product(band(d, d, i, slot)), minus[i + slot // 2])

    inside = [(i, slot) for i in range(rows) for slot in (0, 2) if 0 <= i + slot - 1 < rows]
    hear(1)
    slots[me] = part[...]
    for k in sorted(range(1, n_grow), key=lambda k: -min(k, n_grow - k)):
        pltpu.make_async_remote_copy(
            src_ref=slots.at[me],
            dst_ref=slots.at[me],
            send_sem=trace_send.at[1],
            recv_sem=trace_recv.at[1],
            device_id=at(k),
            device_id_type=MESH,
        ).start()
    sent3 = exchange(3, edge.at[2, 0], edge.at[2, 1], whole)
    for i, slot in inside:
        inner(i, slot)

    def finish(i, slot):
        factor = 0.5 if slot == 1 else half_masks[i + slot // 2]
        out[i, slot] = product(band(d, t, i, slot)) * factor

    for i in range(rows):
        for slot in range(3):
            if 0 < i < last or (i, slot) in ((0, 2), (last, 0)):
                finish(i, slot)
    arrived(sent2, 2, upper)
    take_diagonal(d, 2, 0, -1)
    take_diagonal(d, 2, 1, rows)
    x = product([((d, -1, 1), (d, -1, 2)), ((d, -1, 2), (d, 0, 1))])
    scaled(t, -1, 2, x, minus[0])
    x = product([((d, rows, 1), (d, rows, 0)), ((d, rows, 0), (d, last, 1))])
    scaled(t, rows, 0, x, minus[rows])
    scaled(t, 0, 0, product(band(d, d, 0, 0)), minus[0])
    scaled(t, last, 2, product(band(d, d, last, 2)), minus[rows])
    finish(0, 1)
    finish(last, 1)
    arrived(sent3, 3, whole)
    take_diagonal(t, 3, 0, -1)
    take_diagonal(t, 3, 1, rows)
    finish(0, 0)
    finish(last, 2)

    for copy in sent0 + sent1 + sent2 + sent3:
        copy.wait_send()
    others = slots.at[pl.ds(0, n_grow - 1)]
    for sem in (trace_send.at[1], trace_recv.at[1]):
        pltpu.make_async_copy(others, others, sem).wait()
    order = float(rows * n_grow * edge_size)
    occupation[0] = (order + jnp.sum(slots[...])) / (2.0 * order)


def local(n_grow, hamiltonian, pattern, potential):
    rows, slot_count, edge_size, _ = hamiltonian.shape
    full = (rows + 2, slot_count, edge_size, edge_size)
    block = (edge_size, edge_size)
    splits = [pltpu.VMEM(full, BF16) for _ in range(8)]
    steps = max(1, (n_grow // 2).bit_length())
    return pl.pallas_call(
        functools.partial(kernel, n_grow),
        out_shape=(
            pltpu.VMEM(hamiltonian.shape, F32),
            pltpu.SMEM((1,), F32),
        ),
        in_specs=[
            pl.BlockSpec(memory_space=pltpu.HBM),
            pl.BlockSpec(memory_space=pltpu.SMEM),
            pl.BlockSpec(memory_space=pltpu.HBM),
        ],
        out_specs=(
            pl.BlockSpec(memory_space=pltpu.VMEM),
            pl.BlockSpec(memory_space=pltpu.SMEM),
        ),
        scratch_shapes=[
            pltpu.SMEM(pattern.shape[::-1], jnp.int32),
            pltpu.VMEM(hamiltonian.shape, F32),
            *splits,
            pltpu.VMEM((4, 2, *block), F32),
            pltpu.VMEM((3, 2, *block), F32),
            pltpu.VMEM((1, 128), F32),
            pltpu.VMEM((1, 128), F32),
            pltpu.VMEM((n_grow, 1, 128), F32),
            pltpu.SemaphoreType.DMA((rows + 1,)),
            pltpu.SemaphoreType.DMA((4, 2, 2)),
            pltpu.SemaphoreType.DMA((4, 2, 2)),
            pltpu.SemaphoreType.DMA((2,)),
            pltpu.SemaphoreType.DMA((2,)),
            pltpu.SemaphoreType.REGULAR((steps,)),
        ],
        compiler_params=pltpu.CompilerParams(
            collective_id=0,
            has_side_effects=True,
            vmem_limit_bytes=50 * 1024 * 1024,
        ),
        cost_estimate=pl.CostEstimate(
            flops=2 * 166 * 3 * edge_size**3,
            bytes_accessed=2 * 4 * rows * slot_count * edge_size**2,
            transcendentals=0,
        ),
    )(pattern.T, potential, hamiltonian)


def solution(mesh):
    in_specs = (P(("reps", "grow"), None, None, None), P(), P("reps"))
    out_specs = (P(("reps", "grow"), None, None, None), P("reps"))
    step = functools.partial(local, mesh.shape["grow"])

    def run(hamiltonian, pattern, potential):
        return step(hamiltonian, pattern, potential)

    return jax.shard_map(run, mesh=mesh, in_specs=in_specs, out_specs=out_specs, check_vma=False)
```
